32 devices in a mesh: section: 4 (over x, core), tp: 8 (over z, y).
Axes of the slice: x: 2, y: 2, z: 4, core: 2. Of those that a mesh axis runs over, the one named last changes fastest.
Arguments:
- pending_activation: bfloat16 [4, 128, 4096], P('section'), may hold values from -6 to 6
- admissible_microbatches: bfloat16 [4, 128, 4096], P(None, None, 'tp'), may hold values from -6 to 6
- arrival_plan: int32 [4], replicated, may hold values from 0 to 3, each once
- vanished_hop: int32 [1], replicated, may hold values from 1 to 3
- query_key_value_matrices: bfloat16 [4, 4096, 3, 2048], P('section', None, None, 'tp')
- mixing_projection_matrices: bfloat16 [4, 2048, 4096], P('section', 'tp'), may hold values from -0.125 to 0.125
- normalizer_factors: bfloat16 [4, 4096], P('section'), may hold values from 0.25 to 1.75
Outputs:
- activation_later: bfloat16 [4, 128, 4096], P('section')
- standby_input: bfloat16 [4, 128, 4096], P('section', None, 'tp')
The draws below stay inside these ranges and needn't reach their ends.
Inputs may be any that keep to these rules, and one draw needn't show every extreme that they name: `vanished_hop`: the preempted section is not the first. `arrival_plan`: each micro-batch index once.
All inputs are finite; a program needn't handle non-finite values.
Results may differ from the reference program's by a relative error of at most 0.013.
Values may be sent and summed in bfloat16 or wider, within the bound.
A program may use at most 64 MiB of HBM per device.

```python
import jax
import jax.numpy as jnp
from jax import lax

HIDDEN_SIZE = 4096
HEADS = 16
HD = 128
STRING_LENGTH = 128
TICKS = 3
POOL = 4
LAYER_HOPS = 4


def draw_query_key_value_matrices(key, part):
    base = jax.random.normal(key, (LAYER_HOPS, HIDDEN_SIZE, 3, HEADS * HD), jnp.float32) * HIDDEN_SIZE ** (-0.5)
    return base.astype(jnp.bfloat16)


def level_of(stream_key, dims, pieces, low, high):
    loudness = 1.0
    for position, shards_of in pieces:
        draws = jax.random.uniform(jax.random.fold_in(jax.random.fold_in(stream_key, 6), position), (shards_of,), jnp.float32, low / len(pieces), high / len(pieces))
        loudness = loudness * jnp.repeat(jnp.exp(draws), dims[position] // shards_of).reshape((-1,) + (1,) * (len(dims) - 1 - position))
    return loudness


def bell_draw(rng, dims, width, limit, cuts=(), held_as=jnp.bfloat16):
    array = jax.random.normal(rng, dims, jnp.float32) * width
    if len(cuts) > 0:
        array = level_of(rng, dims, cuts, -0.22, 0.18) * array
    return jnp.clip(array, min=-limit, max=limit).astype(held_as)


def setup_inputs(seed: int = 0) -> dict:
    arg_keys = jax.random.split(jax.random.key(seed), 8)
    pending_activation = bell_draw(arg_keys[0], (LAYER_HOPS, STRING_LENGTH, HIDDEN_SIZE), 1.0, 6.0, ((0, 4),))
    admissible_microbatches = bell_draw(arg_keys[1], (POOL, STRING_LENGTH, HIDDEN_SIZE), 1.0, 6.0, ((2, 8),))
    arrival_plan = jax.random.permutation(arg_keys[2], POOL).astype(jnp.int32)
    vanished_hop = jax.random.randint(arg_keys[3], (1,), 1, LAYER_HOPS).astype(jnp.int32)
    query_key_value_matrices = draw_query_key_value_matrices(jax.random.fold_in(arg_keys[7], 71), 0)
    mixing_projection_matrices = bell_draw(arg_keys[5], (LAYER_HOPS, HEADS * HD, HIDDEN_SIZE), (HEADS * HD) ** -0.5, 0.125, ((0, 4), (1, 8)))
    normalizer_factors = jnp.clip(1.0 + 0.15 * jax.random.normal(arg_keys[6], (LAYER_HOPS, HIDDEN_SIZE), jnp.float32), 0.25, 1.75).astype(jnp.bfloat16)
    return dict(pending_activation=pending_activation, admissible_microbatches=admissible_microbatches, arrival_plan=arrival_plan, vanished_hop=vanished_hop, query_key_value_matrices=query_key_value_matrices, mixing_projection_matrices=mixing_projection_matrices, normalizer_factors=normalizer_factors)


NORM_EPS = 1e-05

def layer_norm(x_rows, scale_row):
    widened = x_rows.astype(jnp.float32)
    row_mean = lax.optimization_barrier(jnp.mean(widened, axis=-1, keepdims=True))
    centered = widened - row_mean
    row_var = lax.optimization_barrier(jnp.mean(centered * centered, axis=-1, keepdims=True))
    return (centered * lax.rsqrt(row_var + NORM_EPS) * scale_row.astype(jnp.float32)).astype(jnp.bfloat16)

def attend(normed, w_in, w_out):
    row_count = normed.shape[0]
    col_count = w_in.shape[2]
    head_count = col_count // HD
    projected = jnp.dot(normed, w_in.reshape(w_in.shape[0], 3 * col_count), preferred_element_type=jnp.float32)
    projected = projected.astype(jnp.bfloat16).reshape(row_count, 3, head_count, HD)
    queries = projected[:, 0].astype(jnp.float32)
    key_rows = projected[:, 1].astype(jnp.float32)
    values = projected[:, 2].astype(jnp.float32)
    scores = jnp.einsum('qhd,khd->hqk', queries, key_rows) * HD ** (-0.5)
    causal = jnp.arange(row_count)[:, None] >= jnp.arange(row_count)[None, :]
    scores = jnp.where(causal[None], scores, -jnp.inf)
    row_max = lax.optimization_barrier(jnp.max(scores, axis=-1, keepdims=True))
    weights = jnp.exp(scores - row_max)
    probs = (weights / lax.optimization_barrier(jnp.sum(weights, axis=-1, keepdims=True))).astype(jnp.bfloat16)
    context = jnp.einsum('hqk,khd->qhd', probs.astype(jnp.float32), values)
    context = context.astype(jnp.bfloat16).reshape(row_count, col_count)
    return jnp.dot(context, w_out, preferred_element_type=jnp.float32)

def section_layer(x_rows, w_in, w_out, scale_row):
    branch = attend(layer_norm(x_rows, scale_row), w_in, w_out)
    return (x_rows.astype(jnp.float32) + branch).astype(jnp.bfloat16)

def reference(pending_activation, admissible_microbatches, arrival_plan, vanished_hop, query_key_value_matrices, mixing_projection_matrices, normalizer_factors):
    lost_at = vanished_hop[0]
    section_ids = jnp.arange(LAYER_HOPS)[:, None, None]
    activation_later = pending_activation
    spares = None
    for tick_index in range(TICKS):
        outputs = lax.map(lambda operands: section_layer(*operands), (activation_later, query_key_value_matrices, mixing_projection_matrices, normalizer_factors))
        if tick_index == TICKS - 1:
            spares = lax.map(lambda operands: section_layer(*operands), (outputs, jnp.roll(query_key_value_matrices, -1, axis=0), jnp.roll(mixing_projection_matrices, -1, axis=0), jnp.roll(normalizer_factors, -1, axis=0)))
            redone = lax.dynamic_index_in_dim(spares, lost_at - 1, 0, keepdims=False)
        else:
            earlier = lax.dynamic_index_in_dim(outputs, lost_at - 1, 0, keepdims=False)
            redone = section_layer(earlier, lax.dynamic_index_in_dim(query_key_value_matrices, lost_at, 0, keepdims=False), lax.dynamic_index_in_dim(mixing_projection_matrices, lost_at, 0, keepdims=False), lax.dynamic_index_in_dim(normalizer_factors, lost_at, 0, keepdims=False))
        outputs = lax.dynamic_update_index_in_dim(outputs, redone, lost_at - 1, 0)
        entering = lax.dynamic_index_in_dim(admissible_microbatches, arrival_plan[tick_index], 0, keepdims=True)
        shifted = jnp.concatenate([entering, outputs[:-1]], axis=0)
        activation_later = jnp.where(section_ids == lost_at, jnp.zeros_like(shifted), jnp.where(section_ids == lost_at + 1, redone[None], shifted))
    standby_input = jnp.roll(spares, 2, axis=0)
    return (activation_later, standby_input)
```

```python
import functools

import jax
import jax.numpy as jnp
from jax import lax
from jax.experimental import pallas as pl
from jax.experimental.pallas import tpu as pltpu
from jax.sharding import PartitionSpec as P

HD = 128
TICKS = 3
NORM_EPS = 1e-05
MESH = pl.DeviceIdType.MESH
PIECES = 4
HALVES = 2
LANES = 128


def relay_kernel(
    sections, nz, ny,
    lost_ref, plan_ref, pend_hbm, pool_hbm, win_hbm, wout_hbm, gain_ref,
    later_hbm, standby_hbm,
    win_ref, wout_ref, pool_buf, x_buf, y_buf, pivot, sum_1, sum_2, csum, acc, qkv, ctx,
    part, own_part, ry_buf, zs_buf, rz_buf, fwd_buf, spare_buf, spare_in,
    w_sem, x_sem, io_sem, fw_s, ag_zs, ag_zr, ag_ys, ag_yr, rs_zs, rs_zr, rs_ys, rs_yr, sp_s, sp_r,
):
    steps = TICKS + 2
    s = lax.axis_index("section")
    me = lax.axis_index("tp")
    z, y = me // ny, me % ny
    nxt, prv = (s + 1) % sections, (s + sections - 1) % sections
    lost = lost_ref[0]
    devices = nz * ny
    rows, width = x_buf.shape[2], x_buf.shape[3]
    cols = wout_ref.shape[0]
    heads = cols // HD
    half = rows // HALVES
    per_half = PIECES // HALVES
    count = float(devices * width)
    far = list(range(nz - 1, -1, -1))

    def partner(at, mask):
        bit = 1
        while bit <= mask:
            if mask & bit:
                at = at + bit - 2 * bit * ((at // bit) % 2)
            bit *= 2
        return at

    def tp_at(dz, dy):
        return partner(z, dz) * ny + partner(y, dy)

    def columns(j):
        return pl.ds(pl.multiple_of(j * width, LANES), width)

    def win_copy(j):
        return pltpu.make_async_copy(win_hbm.at[:, columns(j), :], win_ref.at[:, columns(j), :], w_sem.at[j])

    def pend_copy(j):
        return pltpu.make_async_copy(pend_hbm.at[0, :, columns(j)], x_buf.at[0, j], x_sem.at[j])

    wout_copy = pltpu.make_async_copy(wout_hbm, wout_ref, io_sem.at[0])
    pool_copy = pltpu.make_async_copy(pool_hbm, pool_buf, io_sem.at[1])
    pool_copy.start()
    for j in range(devices):
        pend_copy(j).start()
        win_copy(j).start()
    wout_copy.start()

    barrier = pltpu.get_barrier_semaphore()
    for dz in range(nz):
        if dz:
            pl.semaphore_signal(barrier, inc=1, device_id={"section": s, "tp": tp_at(dz, 0)}, device_id_type=MESH)
        pl.semaphore_signal(barrier, inc=1, device_id={"section": nxt, "tp": tp_at(dz, 0)}, device_id_type=MESH)
        pl.semaphore_signal(barrier, inc=1, device_id={"section": prv, "tp": tp_at(dz, 0)}, device_id_type=MESH)
    for dy in range(1, ny):
        pl.semaphore_signal(barrier, inc=1, device_id={"section": s, "tp": tp_at(0, dy)}, device_id_type=MESH)
    pl.semaphore_wait(barrier, 3 * nz + ny - 2)

    def copy_to(src, dst, send, recv, section, tp):
        return pltpu.make_async_remote_copy(
            src_ref=src, dst_ref=dst, send_sem=send, recv_sem=recv,
            device_id={"section": section, "tp": tp}, device_id_type=MESH,
        )

    def span(h):
        return pl.ds(h * (rows // PIECES), rows // PIECES)

    def pick(cond, a, b):
        return jnp.where(jnp.full(a.shape, cond), a, b)

    def needed(section, n):
        tail = (n <= TICKS) | (section > 2) | (section == 0)
        live = (section + TICKS - 1 >= n) | ((section == 0) & (n == TICKS + 1))
        if sections <= TICKS + 1:
            live = live & ((section != sections - 1) | (n != TICKS - 1))
        return live & tail

    def passes(section, n):
        layered = needed(section, n) & (n > 0) & ((section > 0) | (n == TICKS + 1))
        return layered | ((section > 1) & (n == TICKS + 1))

    def pooled(n):
        return (s == 0) & (((n > 0) & (n < TICKS)) | (n == steps))

    def small(n):
        return (n < s) if sections <= TICKS + 1 else (n < 0)

    def when_full(n, h, body):
        if h == 0:
            body()
        else:
            pl.when(jnp.logical_not(small(n)))(body)

    def z_copy(n, h, dz, slot):
        block = x_buf.at[n, slot, span(h)]
        return copy_to(block, block, ag_zs.at[n - 1], ag_zr.at[n - 1, h, dz], s, tp_at(dz, 0))

    def y_copy(n, h, dz, dy, slot):
        block = x_buf.at[n, slot, span(h)]
        return copy_to(block, block, ag_ys.at[n - 1], ag_yr.at[n - 1, h, dz, dy - 1], s, tp_at(0, dy))

    def fwd_copy(n, h, dz):
        return copy_to(
            fwd_buf.at[n, span(h)], x_buf.at[n + 1, me, span(h)],
            fw_s.at[n], ag_zr.at[n, h, dz], nxt, tp_at(dz, 0),
        )

    def spare_copy(h):
        return copy_to(spare_buf.at[span(h)], spare_in.at[span(h)], sp_s.at[0], sp_r.at[h], nxt, me)

    def sent(ref, sem):
        copy_to(ref, ref, sem, sp_r.at[0], nxt, me).wait_send()

    def sent_blocks(n, blocks, sem):
        @pl.when(jnp.logical_not(small(n)))
        def _():
            sent(x_buf.at[n, pl.ds(0, blocks)], sem)

        if sections <= TICKS + 1:
            @pl.when(small(n))
            def _():
                sent(x_buf.at[n, pl.ds(0, blocks), span(0)], sem)

    def later_copy(j):
        return pltpu.make_async_copy(x_buf.at[steps, j], later_hbm.at[0, :, columns(j)], x_sem.at[j])

    def pool_start(n, tick):
        x_buf[n, me] = pool_buf[plan_ref[tick]]
        for h in range(PIECES):
            for dz in far[:-1]:
                z_copy(n, h, dz, me).start()
            for dy in range(1, ny):
                y_copy(n, h, 0, dy, me).start()

    def forward(n, h, first):
        for dz in range(first, nz):
            z_copy(n, h, dz, tp_at(dz, 0)).wait_recv()
            for dy in range(1, ny):
                y_copy(n, h, dz, dy, tp_at(dz, 0)).start()

    def pool_forward(n):
        for h in range(PIECES):
            forward(n, h, 1)

    def forward_all(n, pieces):
        for h in pieces:
            when_full(n, h, functools.partial(forward, n, h, 0))

    def arrive(n, h, dz):
        for dy in range(1, ny):
            y_copy(n, h, dz, dy, tp_at(dz, dy)).wait_recv()

    def arrive_all(n):
        for h in range(PIECES):
            for dz in range(nz):
                arrive(n, h, dz)

    def blank(n):
        if sections <= TICKS + 1:
            @pl.when(small(n))
            def _():
                deep = rows // PIECES
                for j in range(devices):
                    x_buf[n, j, deep:] = jnp.zeros((rows - deep, width), jnp.bfloat16)

    def tally(xf, at, base):
        s_1 = jnp.zeros((xf.shape[0], LANES), jnp.float32)
        s_2 = jnp.zeros((xf.shape[0], LANES), jnp.float32)
        for c in range(width // LANES):
            d = xf[:, c * LANES:(c + 1) * LANES] - base
            s_1 = s_1 + d
            s_2 = s_2 + d * d
        sum_1[at] += s_1
        sum_2[at] += s_2

    def open_rows(xf, at):
        shape = (xf.shape[0], LANES)
        pivot[at] = jnp.broadcast_to(jnp.sum(xf, axis=-1, keepdims=True) * (1.0 / width), shape)
        sum_1[at] = jnp.zeros(shape, jnp.float32)
        sum_2[at] = jnp.zeros(shape, jnp.float32)

    every = pl.ds(0, rows)

    def first_rows(j, carry):
        pend_copy(j).wait()
        rows_j = x_buf[0, j]
        rows_j = pick((s == lost) | small(0), jnp.zeros_like(rows_j), rows_j)
        x_buf[0, j] = rows_j
        xf = rows_j.astype(jnp.float32)

        @pl.when(j == 0)
        def _():
            open_rows(xf, every)
            acc[...] = jnp.zeros_like(acc)
            csum[...] = jnp.zeros_like(csum)

        tally(xf, every, pivot[...])
        gain = jnp.broadcast_to(gain_ref[:, columns(j)].astype(jnp.float32), (LANES, width)).T
        gain = jnp.concatenate([gain] * (cols // LANES), axis=1)
        ones = jnp.ones((8, width), jnp.bfloat16)
        win_copy(j).wait()
        for i in range(3):
            scaled = (win_ref[i, columns(j), :].astype(jnp.float32) * gain).astype(jnp.bfloat16)
            win_ref[i, columns(j), :] = scaled
            at = slice(i * cols, (i + 1) * cols)
            csum[:, at] += jnp.dot(ones, scaled, preferred_element_type=jnp.float32)
            acc[:, at] += jnp.dot(rows_j, scaled, preferred_element_type=jnp.float32)
        return carry

    def unit(n, r, dz, dy):
        j = tp_at(dz, dy)
        at = pl.ds(r * half, half)
        block = x_buf[n, j, at]
        xf = block.astype(jnp.float32)
        if dz == 0 and dy == 0:
            open_rows(xf, at)
        tally(xf, at, pivot[at])
        for i in range(3):
            product = jnp.dot(block, win_ref[i, columns(j), :], preferred_element_type=jnp.float32)
            if dz == 0 and dy == 0:
                acc[at, i * cols:(i + 1) * cols] = product
            else:
                acc[at, i * cols:(i + 1) * cols] += product

    def gather_project(n):
        handed = passes(s, n)

        def take(r):
            @pl.when(handed)
            def _():
                forward_all(n, range(r * per_half, (r + 1) * per_half))

        def near(r):
            for dz in range(nz):
                unit(n, r, dz, 0)

        def across(r):
            for dz in range(nz):
                for h in range(r * per_half, (r + 1) * per_half):
                    when_full(n, h, functools.partial(arrive, n, h, dz))
                for dy in range(1, ny):
                    unit(n, r, dz, dy)

        blank(n)
        take(0)
        near(0)
        for r in range(1, HALVES):
            take(r)
            across(r - 1)
            near(r)
        across(HALVES - 1)

    def attend():
        m = jnp.sum(sum_1[...], axis=-1, keepdims=True) * (1.0 / count)
        var = jnp.maximum(jnp.sum(sum_2[...], axis=-1, keepdims=True) * (1.0 / count) - m * m, 0.0)
        mean = pivot[:, 0:1] + m
        rstd = lax.rsqrt(var + NORM_EPS)
        qkv[...] = ((acc[...] - mean * csum[0:1, :]) * rstd).astype(jnp.bfloat16)
        causal = lax.broadcasted_iota(jnp.int32, (rows, rows), 0) >= lax.broadcasted_iota(jnp.int32, (rows, rows), 1)
        for h in range(heads):
            q = qkv[:, h * HD:(h + 1) * HD]
            k = qkv[:, cols + h * HD:cols + (h + 1) * HD]
            v = qkv[:, 2 * cols + h * HD:2 * cols + (h + 1) * HD]
            scores = lax.dot_general(q, k, (((1,), (1,)), ((), ())), preferred_element_type=jnp.float32)
            scores = jnp.where(causal, scores * HD ** (-0.5), -jnp.inf)
            weights = jnp.exp(scores - jnp.max(scores, axis=-1, keepdims=True))
            probs = (weights / jnp.sum(weights, axis=-1, keepdims=True)).astype(jnp.bfloat16)
            ctx[:, h * HD:(h + 1) * HD] = jnp.dot(probs, v, preferred_element_type=jnp.float32).astype(jnp.bfloat16)

    def settled(section, h):
        early = (section < lost) | (section - TICKS + 1 > lost)
        return pick(early, y_buf[TICKS - 1, span(h)], y_buf[TICKS, span(h)])

    def send_spare(h):
        early = (s - 1 < lost) | (s - TICKS > lost)
        spare = pick(early, y_buf[TICKS, span(h)], y_buf[TICKS + 1, span(h)])
        spare = pick(s - 1 == lost, y_buf[1, span(h)], spare)
        spare_buf[span(h)] = pick(s == 0, y_buf[TICKS + 1, span(h)], spare)
        spare_copy(h).start()

    def write_later():
        @pl.when(s == 1)
        def _():
            for j in range(devices):
                rows_j = x_buf[TICKS, j]
                x_buf[steps, j] = pick(s == lost, jnp.zeros_like(rows_j), rows_j)

        @pl.when(s > 1)
        def _():
            behind = s - 1
            early = (behind != lost) & ((behind < lost) | (behind - TICKS + 1 > lost))
            for j in range(devices):
                rows_j = pick(early, x_buf[TICKS, j], x_buf[TICKS + 1, j])
                x_buf[steps, j] = pick(s == lost, jnp.zeros_like(rows_j), rows_j)

        @pl.when(s > 0)
        def _():
            for j in range(devices):
                later_copy(j).start()

    def project_out(n):
        def partial_for(tp):
            return jnp.dot(ctx[...], wout_ref[:, columns(tp)], preferred_element_type=jnp.float32)

        turn = n % 3
        def crossed(dy, h):
            return copy_to(part.at[dy - 1, :, span(h)], ry_buf.at[turn, dy - 1, :, span(h)],
                           rs_ys.at[0], rs_yr.at[turn, h, dy - 1], s, tp_at(0, dy))

        def summed(dz, h):
            return copy_to(zs_buf.at[dz - 1, span(h)], rz_buf.at[turn, dz - 1, span(h)],
                           rs_zs.at[0], rs_zr.at[turn, h, dz - 1], s, tp_at(dz, 0))

        def cross(h):
            for dy in range(1, ny):
                crossed(dy, h).start()

        for dz in far:
            for dy in range(1, ny):
                part[dy - 1, dz] = partial_for(tp_at(dz, dy)).astype(jnp.bfloat16)
        for h in range(PIECES):
            when_full(n, h, functools.partial(cross, h))

        @pl.when((s == 0) & (n == 0))
        def _():
            pool_forward(1)

        for dz in far:
            own_part[dz] = partial_for(tp_at(dz, 0))

        @pl.when(n == TICKS + 1)
        def _():
            write_later()

        def over_y(h):
            for dy in range(1, ny):
                crossed(dy, h).wait_recv()
            for dz in far:
                total = own_part[dz, span(h)]
                for dy in range(1, ny):
                    total = total + ry_buf[turn, dy - 1, dz, span(h)].astype(jnp.float32)
                if dz:
                    zs_buf[dz - 1, span(h)] = total.astype(jnp.bfloat16)
                    summed(dz, h).start()
                else:
                    own_part[0, span(h)] = total

        def over_z(h):
            total = own_part[0, span(h)]
            for dz in range(1, nz):
                summed(dz, h).wait_recv()
                total = total + rz_buf[turn, dz - 1, span(h)].astype(jnp.float32)
            y_buf[n, span(h)] = (x_buf[n, me, span(h)].astype(jnp.float32) + total).astype(jnp.bfloat16)

            @pl.when((n < steps - 1) & passes(nxt, n + 1))
            def _():
                fwd_buf[n, span(h)] = y_buf[n, span(h)]

                @pl.when((n == TICKS) & (s == sections - 1))
                def _():
                    fwd_buf[n, span(h)] = pick(s == lost, y_buf[0, span(h)], settled(s, h))

                for dz in far:
                    fwd_copy(n, h, dz).start()

            @pl.when(n == TICKS + 1)
            def _():
                send_spare(h)

        for h in range(PIECES):
            when_full(n, h, functools.partial(over_y, h))
            if h == PIECES - 2:
                over_z(0)
        for h in range(1, PIECES):
            when_full(n, h, functools.partial(over_z, h))

        @pl.when(jnp.logical_not(small(n)))
        def _():
            sent(part, rs_ys.at[0])
            sent(zs_buf, rs_zs.at[0])

        if sections <= TICKS + 1:
            @pl.when(small(n))
            def _():
                for h in range(1, PIECES):
                    y_buf[n, span(h)] = y_buf[n, span(0)]
                sent(part.at[:, :, span(0)], rs_ys.at[0])
                sent(zs_buf.at[:, span(0)], rs_zs.at[0])

    def step(n, carry):
        @pl.when(needed(s, n))
        def _():
            @pl.when(n == 0)
            def _():
                @pl.when(s == 0)
                def _():
                    pool_copy.wait()
                    pool_start(1, 0)

                lax.fori_loop(0, devices, first_rows, 0)
                wout_copy.wait()

            @pl.when(n > 0)
            def _():
                gather_project(n)

            attend()
            project_out(n)

            @pl.when((s == 0) & (n == 1))
            def _():
                pool_start(2, 1)
                pool_forward(2)

        @pl.when(jnp.logical_not(needed(s, n)))
        def _():
            y_buf[n] = jnp.zeros((rows, width), jnp.bfloat16)

            @pl.when((s == 0) & (n == TICKS))
            def _():
                pool_start(steps, TICKS - 1)
                pool_forward(steps)
                arrive_all(steps)
                for j in range(devices):
                    later_copy(j).start()

            @pl.when(n == TICKS + 1)
            def _():
                for h in range(PIECES):
                    send_spare(h)

                @pl.when(passes(s, n))
                def _():
                    forward_all(n, range(PIECES))
                    arrive_all(n)

                write_later()

        return carry

    @pl.when(s > 0)
    def _():
        pool_copy.wait()

    lax.fori_loop(0, steps, step, 0)

    def drain(n, carry):
        @pl.when(passes(nxt, n) & (n < steps))
        def _():
            sent_blocks(n - 1, nz, fw_s.at[n - 1])

        @pl.when(pooled(n))
        def _():
            sent(x_buf.at[n, pl.ds(0, nz - 1)], ag_zs.at[n - 1])

        @pl.when(pooled(n) | (passes(s, n) & (n < steps)))
        def _():
            sent_blocks(n, nz * (ny - 1), ag_ys.at[n - 1])

        return carry

    def standby_copy(h):
        return pltpu.make_async_copy(spare_in.at[span(h)], standby_hbm.at[0, span(h), :], w_sem.at[h])

    for h in range(PIECES):
        spare_copy(h).wait_recv()
        standby_copy(h).start()
    lax.fori_loop(1, steps + 1, drain, 0)
    for j in range(devices):
        later_copy(j).wait()
    sent(spare_buf, sp_s.at[0])
    for h in range(PIECES):
        standby_copy(h).wait()


def solution(mesh):
    sections, devices = mesh.shape["section"], mesh.shape["tp"]
    ny = 1
    while (2 * ny) * (2 * ny) <= devices and devices % (2 * ny) == 0:
        ny *= 2
    nz = devices // ny

    def per_device(pend, pool, plan, lost, win, wout, gain):
        rows, hidden = pend.shape[1], pend.shape[2]
        width = hidden // devices
        cols = win.shape[3]
        slots = TICKS + 3
        win = jnp.transpose(win[0], (1, 0, 2))
        vmem = pl.BlockSpec(memory_space=pltpu.VMEM)
        smem = pl.BlockSpec(memory_space=pltpu.SMEM)
        hbm = pl.BlockSpec(memory_space=pl.ANY)
        bf = functools.partial(pltpu.VMEM, dtype=jnp.bfloat16)
        fl = functools.partial(pltpu.VMEM, dtype=jnp.float32)
        dma = pltpu.SemaphoreType.DMA
        return pl.pallas_call(
            functools.partial(relay_kernel, sections, nz, ny),
            out_shape=(
                jax.ShapeDtypeStruct((1, rows, hidden), jnp.bfloat16),
                jax.ShapeDtypeStruct((1, rows, width), jnp.bfloat16),
            ),
            in_specs=[smem, smem, hbm, hbm, hbm, hbm, vmem],
            out_specs=(hbm, hbm),
            scratch_shapes=[
                bf((3, hidden, cols)),
                bf((cols, hidden)),
                bf(pool.shape),
                bf((slots, devices, rows, width)),
                bf((slots, rows, width)),
                fl((rows, LANES)), fl((rows, LANES)), fl((rows, LANES)),
                fl((8, 3 * cols)),
                fl((rows, 3 * cols)),
                bf((rows, 3 * cols)),
                bf((rows, cols)),
                bf((ny - 1, nz, rows, width)),
                fl((nz, rows, width)),
                bf((3, ny - 1, nz, rows, width)),
                bf((nz - 1, rows, width)),
                bf((3, nz - 1, rows, width)),
                bf((slots, rows, width)),
                bf((rows, width)),
                bf((rows, width)),
                dma((devices,)), dma((devices,)), dma((2,)),
                dma((slots - 1,)), dma((slots - 1,)), dma((slots - 1, PIECES, nz)),
                dma((slots - 1,)), dma((slots - 1, PIECES, nz, ny - 1)),
                dma((1,)), dma((3, PIECES, nz - 1)), dma((1,)), dma((3, PIECES, ny - 1)),
                dma((1,)), dma((PIECES,)),
            ],
            compiler_params=pltpu.CompilerParams(
                collective_id=0, has_side_effects=True, vmem_limit_bytes=60 * 1024 * 1024
            ),
        )(lost, plan, pend, pool, win, wout[0], gain)

    placed = (
        P("section", None, None),
        P(None, None, "tp"),
        P(),
        P(),
        P("section", None, None, "tp"),
        P("section", "tp", None),
        P("section", None),
    )
    return jax.shard_map(
        per_device,
        mesh=mesh,
        in_specs=placed,
        out_specs=(P("section", None, None), P("section", None, "tp")),
        check_vma=False,
    )
```

```python
import functools

import jax
import jax.numpy as jnp
from jax import lax
from jax.experimental import pallas as pl
from jax.experimental.pallas import tpu as pltpu
from jax.sharding import PartitionSpec as P

HD = 128
TICKS = 3
NORM_EPS = 1e-05
MESH = pl.DeviceIdType.MESH
PIECES = 4
HALVES = 2
LANES = 128


def relay_kernel(
    sections, nz, ny,
    lost_ref, plan_ref, pend_hbm, pool_hbm, win_hbm, wout_hbm, gain_ref,
    later_hbm, standby_hbm,
    win_ref, wout_ref, pool_buf, x_buf, y_buf, pivot, sum_1, sum_2, csum, acc, qkv, ctx,
    part, own_part, ry_buf, zs_buf, rz_buf, fwd_buf, spare_buf, spare_in,
    w_sem, x_sem, io_sem, fw_s, ag_zs, ag_zr, ag_ys, ag_yr, rs_zs, rs_zr, rs_ys, rs_yr, sp_s, sp_r, turn_sem,
):
    steps = TICKS + 2
    s = lax.axis_index("section")
    me = lax.axis_index("tp")
    z, y = me // ny, me % ny
    nxt, prv = (s + 1) % sections, (s + sections - 1) % sections
    lost = lost_ref[0]
    devices = nz * ny
    rows, width = x_buf.shape[2], x_buf.shape[3]
    cols = wout_ref.shape[0]
    heads = cols // HD
    half = rows // HALVES
    per_half = PIECES // HALVES
    count = float(devices * width)
    far = list(range(nz - 1, -1, -1))

    def partner(at, mask):
        bit = 1
        while bit <= mask:
            if mask & bit:
                at = at + bit - 2 * bit * ((at // bit) % 2)
            bit *= 2
        return at

    def tp_at(dz, dy):
        return partner(z, dz) * ny + partner(y, dy)

    def columns(j):
        return pl.ds(pl.multiple_of(j * width, LANES), width)

    def win_copy(j):
        return pltpu.make_async_copy(win_hbm.at[:, columns(j), :], win_ref.at[:, columns(j), :], w_sem.at[j])

    def pend_copy(j):
        return pltpu.make_async_copy(pend_hbm.at[0, :, columns(j)], x_buf.at[0, j], x_sem.at[j])

    wout_copy = pltpu.make_async_copy(wout_hbm, wout_ref, io_sem.at[0])
    pool_copy = pltpu.make_async_copy(pool_hbm, pool_buf, io_sem.at[1])
    pool_copy.start()
    for j in range(devices):
        pend_copy(j).start()
        win_copy(j).start()
    wout_copy.start()

    barrier = pltpu.get_barrier_semaphore()
    for dz in range(nz):
        if dz:
            pl.semaphore_signal(barrier, inc=1, device_id={"section": s, "tp": tp_at(dz, 0)}, device_id_type=MESH)
        pl.semaphore_signal(barrier, inc=1, device_id={"section": nxt, "tp": tp_at(dz, 0)}, device_id_type=MESH)
        pl.semaphore_signal(barrier, inc=1, device_id={"section": prv, "tp": tp_at(dz, 0)}, device_id_type=MESH)
    for dy in range(1, ny):
        pl.semaphore_signal(barrier, inc=1, device_id={"section": s, "tp": tp_at(0, dy)}, device_id_type=MESH)
    pl.semaphore_wait(barrier, 3 * nz + ny - 2)

    def copy_to(src, dst, send, recv, section, tp):
        return pltpu.make_async_remote_copy(
            src_ref=src, dst_ref=dst, send_sem=send, recv_sem=recv,
            device_id={"section": section, "tp": tp}, device_id_type=MESH,
        )

    def span(h):
        return pl.ds(h * (rows // PIECES), rows // PIECES)

    def pick(cond, a, b):
        return jnp.where(jnp.full(a.shape, cond), a, b)

    def needed(section, n):
        tail = (n <= TICKS) | (section > 2) | (section == 0)
        live = (section + TICKS - 1 >= n) | ((section == 0) & (n == TICKS + 1))
        if sections <= TICKS + 1:
            live = live & ((section != sections - 1) | (n != TICKS - 1))
        return live & tail

    def passes(section, n):
        layered = needed(section, n) & (n > 0) & ((section > 0) | (n == TICKS + 1))
        return layered | ((section > 1) & (n == TICKS + 1))

    def pooled(n):
        return (s == 0) & (((n > 0) & (n < TICKS)) | (n == steps))

    def small(n):
        return (n < s) if sections <= TICKS + 1 else (n < 0)

    def follows(section, n):
        return (section % 2 == 0) & (n > section) & needed(section, n) & needed(section + 1, n)

    pools = list(enumerate(list(range(1, TICKS)) + [steps]))

    def when_full(n, h, body):
        if h == 0:
            body()
        else:
            pl.when(jnp.logical_not(small(n)))(body)

    def z_copy(n, h, dz, slot):
        block = x_buf.at[n, slot, span(h)]
        return copy_to(block, block, ag_zs.at[n - 1], ag_zr.at[n - 1, h, dz], s, tp_at(dz, 0))

    def y_copy(n, h, dz, dy, slot):
        block = x_buf.at[n, slot, span(h)]
        return copy_to(block, block, ag_ys.at[n - 1], ag_yr.at[n - 1, h, dz, dy - 1], s, tp_at(0, dy))

    def fwd_copy(n, h, dz):
        return copy_to(
            fwd_buf.at[n, span(h)], x_buf.at[n + 1, me, span(h)],
            fw_s.at[n], ag_zr.at[n, h, dz], nxt, tp_at(dz, 0),
        )

    def spare_copy(h):
        return copy_to(spare_buf.at[span(h)], spare_in.at[span(h)], sp_s.at[0], sp_r.at[h], nxt, me)

    def sent(ref, sem):
        copy_to(ref, ref, sem, sp_r.at[0], nxt, me).wait_send()

    def sent_blocks(n, blocks, sem):
        @pl.when(jnp.logical_not(small(n)))
        def _():
            sent(x_buf.at[n, pl.ds(0, blocks)], sem)

        if sections <= TICKS + 1:
            @pl.when(small(n))
            def _():
                sent(x_buf.at[n, pl.ds(0, blocks), span(0)], sem)

    def later_copy(j):
        return pltpu.make_async_copy(x_buf.at[steps, j], later_hbm.at[0, :, columns(j)], x_sem.at[j])

    def pool_start(n, tick):
        x_buf[n, me] = pool_buf[plan_ref[tick]]
        for h in range(PIECES):
            for dz in far[:-1]:
                z_copy(n, h, dz, me).start()
            for dy in range(1, ny):
                y_copy(n, h, 0, dy, me).start()

    def forward(n, h, first):
        for dz in range(first, nz):
            z_copy(n, h, dz, tp_at(dz, 0)).wait_recv()
            for dy in range(1, ny):
                y_copy(n, h, dz, dy, tp_at(dz, 0)).start()

    def pool_forward(n):
        for h in range(PIECES):
            forward(n, h, 1)

    def forward_all(n, pieces):
        for h in pieces:
            when_full(n, h, functools.partial(forward, n, h, 0))

    def arrive(n, h, dz):
        for dy in range(1, ny):
            y_copy(n, h, dz, dy, tp_at(dz, dy)).wait_recv()

    def arrive_all(n):
        for h in range(PIECES):
            for dz in range(nz):
                arrive(n, h, dz)

    def blank(n):
        if sections <= TICKS + 1:
            @pl.when(small(n))
            def _():
                deep = rows // PIECES
                for j in range(devices):
                    x_buf[n, j, deep:] = jnp.zeros((rows - deep, width), jnp.bfloat16)

    def tally(xf, at, base):
        s_1 = jnp.zeros((xf.shape[0], LANES), jnp.float32)
        s_2 = jnp.zeros((xf.shape[0], LANES), jnp.float32)
        for c in range(width // LANES):
            d = xf[:, c * LANES:(c + 1) * LANES] - base
            s_1 = s_1 + d
            s_2 = s_2 + d * d
        sum_1[at] += s_1
        sum_2[at] += s_2

    def open_rows(xf, at):
        shape = (xf.shape[0], LANES)
        pivot[at] = jnp.broadcast_to(jnp.sum(xf, axis=-1, keepdims=True) * (1.0 / width), shape)
        sum_1[at] = jnp.zeros(shape, jnp.float32)
        sum_2[at] = jnp.zeros(shape, jnp.float32)

    every = pl.ds(0, rows)

    def first_rows(j, carry):
        pend_copy(j).wait()
        rows_j = x_buf[0, j]
        rows_j = pick((s == lost) | small(0), jnp.zeros_like(rows_j), rows_j)
        x_buf[0, j] = rows_j
        xf = rows_j.astype(jnp.float32)

        @pl.when(j == 0)
        def _():
            open_rows(xf, every)
            acc[...] = jnp.zeros_like(acc)
            csum[...] = jnp.zeros_like(csum)

        tally(xf, every, pivot[...])
        gain = jnp.broadcast_to(gain_ref[:, columns(j)].astype(jnp.float32), (LANES, width)).T
        gain = jnp.concatenate([gain] * (cols // LANES), axis=1)
        ones = jnp.ones((8, width), jnp.bfloat16)
        win_copy(j).wait()
        for i in range(3):
            scaled = (win_ref[i, columns(j), :].astype(jnp.float32) * gain).astype(jnp.bfloat16)
            win_ref[i, columns(j), :] = scaled
            at = slice(i * cols, (i + 1) * cols)
            csum[:, at] += jnp.dot(ones, scaled, preferred_element_type=jnp.float32)
            acc[:, at] += jnp.dot(rows_j, scaled, preferred_element_type=jnp.float32)
        return carry

    def unit(n, r, dz, dy):
        j = tp_at(dz, dy)
        at = pl.ds(r * half, half)
        block = x_buf[n, j, at]
        xf = block.astype(jnp.float32)
        if dz == 0 and dy == 0:
            open_rows(xf, at)
        tally(xf, at, pivot[at])
        for i in range(3):
            product = jnp.dot(block, win_ref[i, columns(j), :], preferred_element_type=jnp.float32)
            if dz == 0 and dy == 0:
                acc[at, i * cols:(i + 1) * cols] = product
            else:
                acc[at, i * cols:(i + 1) * cols] += product

    def gather_project(n):
        handed = passes(s, n)

        def take(r):
            @pl.when(handed)
            def _():
                forward_all(n, range(r * per_half, (r + 1) * per_half))

        def near(r):
            for dz in range(nz):
                unit(n, r, dz, 0)

        def across(r):
            for dz in range(nz):
                for h in range(r * per_half, (r + 1) * per_half):
                    when_full(n, h, functools.partial(arrive, n, h, dz))
                for dy in range(1, ny):
                    unit(n, r, dz, dy)

        blank(n)
        take(0)
        near(0)
        for r in range(1, HALVES):
            take(r)
            across(r - 1)
            near(r)
        across(HALVES - 1)

    def attend():
        m = jnp.sum(sum_1[...], axis=-1, keepdims=True) * (1.0 / count)
        var = jnp.maximum(jnp.sum(sum_2[...], axis=-1, keepdims=True) * (1.0 / count) - m * m, 0.0)
        mean = pivot[:, 0:1] + m
        rstd = lax.rsqrt(var + NORM_EPS)
        qkv[...] = ((acc[...] - mean * csum[0:1, :]) * rstd).astype(jnp.bfloat16)
        causal = lax.broadcasted_iota(jnp.int32, (rows, rows), 0) >= lax.broadcasted_iota(jnp.int32, (rows, rows), 1)
        for h in range(heads):
            q = qkv[:, h * HD:(h + 1) * HD]
            k = qkv[:, cols + h * HD:cols + (h + 1) * HD]
            v = qkv[:, 2 * cols + h * HD:2 * cols + (h + 1) * HD]
            scores = lax.dot_general(q, k, (((1,), (1,)), ((), ())), preferred_element_type=jnp.float32)
            scores = jnp.where(causal, scores * HD ** (-0.5), -jnp.inf)
            weights = jnp.exp(scores - jnp.max(scores, axis=-1, keepdims=True))
            probs = (weights / jnp.sum(weights, axis=-1, keepdims=True)).astype(jnp.bfloat16)
            ctx[:, h * HD:(h + 1) * HD] = jnp.dot(probs, v, preferred_element_type=jnp.float32).astype(jnp.bfloat16)

    def settled(section, h):
        early = (section < lost) | (section - TICKS + 1 > lost)
        return pick(early, y_buf[TICKS - 1, span(h)], y_buf[TICKS, span(h)])

    def send_spare(h):
        early = (s - 1 < lost) | (s - TICKS > lost)
        spare = pick(early, y_buf[TICKS, span(h)], y_buf[TICKS + 1, span(h)])
        spare = pick(s - 1 == lost, y_buf[1, span(h)], spare)
        spare_buf[span(h)] = pick(s == 0, y_buf[TICKS + 1, span(h)], spare)
        spare_copy(h).start()

    def write_later():
        @pl.when(s == 1)
        def _():
            for j in range(devices):
                rows_j = x_buf[TICKS, j]
                x_buf[steps, j] = pick(s == lost, jnp.zeros_like(rows_j), rows_j)

        @pl.when(s > 1)
        def _():
            behind = s - 1
            early = (behind != lost) & ((behind < lost) | (behind - TICKS + 1 > lost))
            for j in range(devices):
                rows_j = pick(early, x_buf[TICKS, j], x_buf[TICKS + 1, j])
                x_buf[steps, j] = pick(s == lost, jnp.zeros_like(rows_j), rows_j)

        @pl.when(s > 0)
        def _():
            for j in range(devices):
                later_copy(j).start()

    def project_out(n):
        def partial_for(tp):
            return jnp.dot(ctx[...], wout_ref[:, columns(tp)], preferred_element_type=jnp.float32)

        turn = n % 3
        def crossed(dy, h):
            return copy_to(part.at[dy - 1, :, span(h)], ry_buf.at[turn, dy - 1, :, span(h)],
                           rs_ys.at[0], rs_yr.at[turn, h, dy - 1], s, tp_at(0, dy))

        def summed(dz, h):
            return copy_to(zs_buf.at[dz - 1, span(h)], rz_buf.at[turn, dz - 1, span(h)],
                           rs_zs.at[0], rs_zr.at[turn, h, dz - 1], s, tp_at(dz, 0))

        def cross(h):
            for dy in range(1, ny):
                crossed(dy, h).start()

        for dz in far:
            for dy in range(1, ny):
                part[dy - 1, dz] = partial_for(tp_at(dz, dy)).astype(jnp.bfloat16)
        if sections <= TICKS + 1:
            @pl.when(follows(s, n))
            def _():
                pl.semaphore_wait(turn_sem, 1)

        for h in range(PIECES):
            when_full(n, h, functools.partial(cross, h))

        for tick, slot in pools:
            pl.when((s == 0) & (n == tick))(functools.partial(pool_forward, slot))

        for dz in far:
            own_part[dz] = partial_for(tp_at(dz, 0))

        @pl.when(n == TICKS + 1)
        def _():
            write_later()

        def over_y(h):
            for dy in range(1, ny):
                crossed(dy, h).wait_recv()
            for dz in far:
                total = own_part[dz, span(h)]
                for dy in range(1, ny):
                    total = total + ry_buf[turn, dy - 1, dz, span(h)].astype(jnp.float32)
                if dz:
                    zs_buf[dz - 1, span(h)] = total.astype(jnp.bfloat16)
                    summed(dz, h).start()
                else:
                    own_part[0, span(h)] = total

        def over_z(h):
            total = own_part[0, span(h)]
            for dz in range(1, nz):
                summed(dz, h).wait_recv()
                total = total + rz_buf[turn, dz - 1, span(h)].astype(jnp.float32)
            y_buf[n, span(h)] = (x_buf[n, me, span(h)].astype(jnp.float32) + total).astype(jnp.bfloat16)

            @pl.when((n < steps - 1) & passes(nxt, n + 1))
            def _():
                fwd_buf[n, span(h)] = y_buf[n, span(h)]

                @pl.when((n == TICKS) & (s == sections - 1))
                def _():
                    fwd_buf[n, span(h)] = pick(s == lost, y_buf[0, span(h)], settled(s, h))

                for dz in far:
                    fwd_copy(n, h, dz).start()

            @pl.when(n == TICKS + 1)
            def _():
                send_spare(h)

        for h in range(PIECES):
            when_full(n, h, functools.partial(over_y, h))
            if h == PIECES - 2:
                over_z(0)
        if sections <= TICKS + 1:
            @pl.when((s % 2 == 1) & follows(s - 1, n))
            def _():
                pl.semaphore_signal(turn_sem, inc=1, device_id={"section": prv, "tp": me}, device_id_type=MESH)

        for h in range(1, PIECES):
            when_full(n, h, functools.partial(over_z, h))

        @pl.when(jnp.logical_not(small(n)))
        def _():
            sent(part, rs_ys.at[0])
            sent(zs_buf, rs_zs.at[0])

        if sections <= TICKS + 1:
            @pl.when(small(n))
            def _():
                for h in range(1, PIECES):
                    y_buf[n, span(h)] = y_buf[n, span(0)]
                sent(part.at[:, :, span(0)], rs_ys.at[0])
                sent(zs_buf.at[:, span(0)], rs_zs.at[0])

    def step(n, carry):
        @pl.when(needed(s, n))
        def _():
            for tick, slot in pools:
                pl.when((s == 0) & (n == tick))(functools.partial(pool_start, slot, tick))

            @pl.when(n == 0)
            def _():
                lax.fori_loop(0, devices, first_rows, 0)
                wout_copy.wait()

            @pl.when(n > 0)
            def _():
                gather_project(n)

            attend()
            project_out(n)

        @pl.when(jnp.logical_not(needed(s, n)))
        def _():
            y_buf[n] = jnp.zeros((rows, width), jnp.bfloat16)

            @pl.when((s == 0) & (n == TICKS))
            def _():
                arrive_all(steps)
                for j in range(devices):
                    later_copy(j).start()

            @pl.when(n == TICKS + 1)
            def _():
                for h in range(PIECES):
                    send_spare(h)

                @pl.when(passes(s, n))
                def _():
                    forward_all(n, range(PIECES))
                    arrive_all(n)

                write_later()

        return carry

    pool_copy.wait()

    lax.fori_loop(0, steps, step, 0)

    def drain(n, carry):
        @pl.when(passes(nxt, n) & (n < steps))
        def _():
            sent_blocks(n - 1, nz, fw_s.at[n - 1])

        @pl.when(pooled(n))
        def _():
            sent(x_buf.at[n, pl.ds(0, nz - 1)], ag_zs.at[n - 1])

        @pl.when(pooled(n) | (passes(s, n) & (n < steps)))
        def _():
            sent_blocks(n, nz * (ny - 1), ag_ys.at[n - 1])

        return carry

    def standby_copy(h):
        return pltpu.make_async_copy(spare_in.at[span(h)], standby_hbm.at[0, span(h), :], w_sem.at[h])

    for h in range(PIECES):
        spare_copy(h).wait_recv()
        standby_copy(h).start()
    lax.fori_loop(1, steps + 1, drain, 0)
    for j in range(devices):
        later_copy(j).wait()
    sent(spare_buf, sp_s.at[0])
    for h in range(PIECES):
        standby_copy(h).wait()


def solution(mesh):
    sections, devices = mesh.shape["section"], mesh.shape["tp"]
    ny = 1
    while (2 * ny) * (2 * ny) <= devices and devices % (2 * ny) == 0:
        ny *= 2
    nz = devices // ny

    def per_device(pend, pool, plan, lost, win, wout, gain):
        rows, hidden = pend.shape[1], pend.shape[2]
        width = hidden // devices
        cols = win.shape[3]
        slots = TICKS + 3
        win = jnp.transpose(win[0], (1, 0, 2))
        vmem = pl.BlockSpec(memory_space=pltpu.VMEM)
        smem = pl.BlockSpec(memory_space=pltpu.SMEM)
        hbm = pl.BlockSpec(memory_space=pl.ANY)
        bf = functools.partial(pltpu.VMEM, dtype=jnp.bfloat16)
        fl = functools.partial(pltpu.VMEM, dtype=jnp.float32)
        dma = pltpu.SemaphoreType.DMA
        return pl.pallas_call(
            functools.partial(relay_kernel, sections, nz, ny),
            out_shape=(
                jax.ShapeDtypeStruct((1, rows, hidden), jnp.bfloat16),
                jax.ShapeDtypeStruct((1, rows, width), jnp.bfloat16),
            ),
            in_specs=[smem, smem, hbm, hbm, hbm, hbm, vmem],
            out_specs=(hbm, hbm),
            scratch_shapes=[
                bf((3, hidden, cols)),
                bf((cols, hidden)),
                bf(pool.shape),
                bf((slots, devices, rows, width)),
                bf((slots, rows, width)),
                fl((rows, LANES)), fl((rows, LANES)), fl((rows, LANES)),
                fl((8, 3 * cols)),
                fl((rows, 3 * cols)),
                bf((rows, 3 * cols)),
                bf((rows, cols)),
                bf((ny - 1, nz, rows, width)),
                fl((nz, rows, width)),
                bf((3, ny - 1, nz, rows, width)),
                bf((nz - 1, rows, width)),
                bf((3, nz - 1, rows, width)),
                bf((slots, rows, width)),
                bf((rows, width)),
                bf((rows, width)),
                dma((devices,)), dma((devices,)), dma((2,)),
                dma((slots - 1,)), dma((slots - 1,)), dma((slots - 1, PIECES, nz)),
                dma((slots - 1,)), dma((slots - 1, PIECES, nz, ny - 1)),
                dma((1,)), dma((3, PIECES, nz - 1)), dma((1,)), dma((3, PIECES, ny - 1)),
                dma((1,)), dma((PIECES,)), pltpu.SemaphoreType.REGULAR,
            ],
            compiler_params=pltpu.CompilerParams(
                collective_id=0, has_side_effects=True, vmem_limit_bytes=60 * 1024 * 1024
            ),
        )(lost, plan, pend, pool, win, wout[0], gain)

    placed = (
        P("section", None, None),
        P(None, None, "tp"),
        P(),
        P(),
        P("section", None, None, "tp"),
        P("section", "tp", None),
        P("section", None),
    )
    return jax.shard_map(
        per_device,
        mesh=mesh,
        in_specs=placed,
        out_specs=(P("section", None, None), P("section", None, "tp")),
        check_vma=False,
    )
```

```python
import functools

import jax
import jax.numpy as jnp
from jax import lax
from jax.experimental import pallas as pl
from jax.experimental.pallas import tpu as pltpu
from jax.sharding import PartitionSpec as P

HD = 128
TICKS = 3
NORM_EPS = 1e-05
MESH = pl.DeviceIdType.MESH
PIECES = 4
HALVES = 2
LANES = 128


def relay_kernel(
    sections, nz, ny,
    lost_ref, plan_ref, pend_hbm, pool_hbm, win_hbm, wout_hbm, gain_ref,
    later_hbm, standby_hbm,
    win_ref, wout_ref, pool_buf, x_buf, y_buf, pivot, sum_1, sum_2, csum, acc, qkv, ctx,
    part, own_part, ry_buf, zs_buf, rz_buf, fwd_buf, spare_buf, spare_in,
    w_sem, x_sem, io_sem, fw_s, ag_zs, ag_zr, ag_ys, ag_yr, rs_zs, rs_zr, rs_ys, rs_yr, sp_s, sp_r, turn_sem,
):
    steps = TICKS + 2
    s = lax.axis_index("section")
    me = lax.axis_index("tp")
    z, y = me // ny, me % ny
    nxt, prv = (s + 1) % sections, (s + sections - 1) % sections
    lost = lost_ref[0]
    devices = nz * ny
    rows, width = x_buf.shape[2], x_buf.shape[3]
    cols = wout_ref.shape[0]
    heads = cols // HD
    half = rows // HALVES
    per_half = PIECES // HALVES
    count = float(devices * width)
    far = list(range(nz - 1, -1, -1))

    def partner(at, mask):
        bit = 1
        while bit <= mask:
            if mask & bit:
                at = at + bit - 2 * bit * ((at // bit) % 2)
            bit *= 2
        return at

    def tp_at(dz, dy):
        return partner(z, dz) * ny + partner(y, dy)

    def columns(j):
        return pl.ds(pl.multiple_of(j * width, LANES), width)

    def win_copy(j):
        return pltpu.make_async_copy(win_hbm.at[:, columns(j), :], win_ref.at[:, columns(j), :], w_sem.at[j])

    def pend_copy(j):
        return pltpu.make_async_copy(pend_hbm.at[0, :, columns(j)], x_buf.at[0, j], x_sem.at[j])

    wout_copy = pltpu.make_async_copy(wout_hbm, wout_ref, io_sem.at[0])
    pool_copy = pltpu.make_async_copy(pool_hbm, pool_buf, io_sem.at[1])
    pool_copy.start()
    for j in range(devices):
        pend_copy(j).start()
        win_copy(j).start()
    wout_copy.start()

    barrier = pltpu.get_barrier_semaphore()
    for dz in range(nz):
        if dz:
            pl.semaphore_signal(barrier, inc=1, device_id={"section": s, "tp": tp_at(dz, 0)}, device_id_type=MESH)
        pl.semaphore_signal(barrier, inc=1, device_id={"section": nxt, "tp": tp_at(dz, 0)}, device_id_type=MESH)
        pl.semaphore_signal(barrier, inc=1, device_id={"section": prv, "tp": tp_at(dz, 0)}, device_id_type=MESH)
    for dy in range(1, ny):
        pl.semaphore_signal(barrier, inc=1, device_id={"section": s, "tp": tp_at(0, dy)}, device_id_type=MESH)
    pl.semaphore_wait(barrier, 3 * nz + ny - 2)

    def copy_to(src, dst, send, recv, section, tp):
        return pltpu.make_async_remote_copy(
            src_ref=src, dst_ref=dst, send_sem=send, recv_sem=recv,
            device_id={"section": section, "tp": tp}, device_id_type=MESH,
        )

    def span(h):
        return pl.ds(h * (rows // PIECES), rows // PIECES)

    def pick(cond, a, b):
        return jnp.where(jnp.full(a.shape, cond), a, b)

    def needed(section, n):
        tail = (n <= TICKS) | (section > 2) | (section == 0)
        live = (section + TICKS - 1 >= n) | ((section == 0) & (n == TICKS + 1))
        if sections <= TICKS + 1:
            live = live & ((section != sections - 1) | (n != TICKS - 1))
        return live & tail

    def passes(section, n):
        layered = needed(section, n) & (n > 0) & ((section > 0) | (n == TICKS + 1))
        return layered | ((section > 1) & (n == TICKS + 1))

    def pooled(n):
        return (s == 0) & (((n > 0) & (n < TICKS)) | (n == steps))

    def small(n):
        return (n < s) if sections <= TICKS + 1 else (n < 0)

    def follows(section, n):
        return (section % 2 == 0) & (n > section) & needed(section, n) & needed(section + 1, n)

    pools = list(enumerate(list(range(1, TICKS)) + [steps]))

    def when_full(n, h, body):
        if h == 0:
            body()
        else:
            pl.when(jnp.logical_not(small(n)))(body)

    def z_copy(n, h, dz, slot):
        block = x_buf.at[n, slot, span(h)]
        return copy_to(block, block, ag_zs.at[n - 1], ag_zr.at[n - 1, h, dz], s, tp_at(dz, 0))

    def y_copy(n, h, dz, dy, slot):
        block = x_buf.at[n, slot, span(h)]
        return copy_to(block, block, ag_ys.at[n - 1], ag_yr.at[n - 1, h, dz, dy - 1], s, tp_at(0, dy))

    def fwd_copy(n, h, dz):
        return copy_to(
            fwd_buf.at[n, span(h)], x_buf.at[n + 1, me, span(h)],
            fw_s.at[n], ag_zr.at[n, h, dz], nxt, tp_at(dz, 0),
        )

    def spare_copy(h):
        return copy_to(spare_buf.at[span(h)], spare_in.at[span(h)], sp_s.at[0], sp_r.at[h], nxt, me)

    def sent(ref, sem):
        copy_to(ref, ref, sem, sp_r.at[0], nxt, me).wait_send()

    def sent_blocks(n, blocks, sem):
        @pl.when(jnp.logical_not(small(n)))
        def _():
            sent(x_buf.at[n, pl.ds(0, blocks)], sem)

        if sections <= TICKS + 1:
            @pl.when(small(n))
            def _():
                sent(x_buf.at[n, pl.ds(0, blocks), span(0)], sem)

    def later_copy(j):
        return pltpu.make_async_copy(x_buf.at[steps, j], later_hbm.at[0, :, columns(j)], x_sem.at[j])

    def pool_start(n, tick):
        x_buf[n, me] = pool_buf[plan_ref[tick]]
        for h in range(PIECES):
            for dz in far[:-1]:
                z_copy(n, h, dz, me).start()
            for dy in range(1, ny):
                y_copy(n, h, 0, dy, me).start()

    def forward(n, h, first):
        for dz in range(first, nz):
            z_copy(n, h, dz, tp_at(dz, 0)).wait_recv()
            for dy in range(1, ny):
                y_copy(n, h, dz, dy, tp_at(dz, 0)).start()

    def pool_forward(n):
        for h in range(PIECES):
            forward(n, h, 1)

    def forward_all(n, pieces):
        for h in pieces:
            when_full(n, h, functools.partial(forward, n, h, 0))

    def arrive(n, h, dz):
        for dy in range(1, ny):
            y_copy(n, h, dz, dy, tp_at(dz, dy)).wait_recv()

    def arrive_all(n):
        for h in range(PIECES):
            for dz in range(nz):
                arrive(n, h, dz)

    def blank(n):
        if sections <= TICKS + 1:
            @pl.when(small(n))
            def _():
                deep = rows // PIECES
                for j in range(devices):
                    x_buf[n, j, deep:] = jnp.zeros((rows - deep, width), jnp.bfloat16)

    def tally(xf, at, base):
        s_1 = jnp.zeros((xf.shape[0], LANES), jnp.float32)
        s_2 = jnp.zeros((xf.shape[0], LANES), jnp.float32)
        for c in range(width // LANES):
            d = xf[:, c * LANES:(c + 1) * LANES] - base
            s_1 = s_1 + d
            s_2 = s_2 + d * d
        sum_1[at] += s_1
        sum_2[at] += s_2

    def open_rows(xf, at):
        shape = (xf.shape[0], LANES)
        pivot[at] = jnp.broadcast_to(jnp.sum(xf, axis=-1, keepdims=True) * (1.0 / width), shape)
        sum_1[at] = jnp.zeros(shape, jnp.float32)
        sum_2[at] = jnp.zeros(shape, jnp.float32)

    every = pl.ds(0, rows)

    def first_rows(j, carry):
        pend_copy(j).wait()
        rows_j = x_buf[0, j]
        rows_j = pick((s == lost) | small(0), jnp.zeros_like(rows_j), rows_j)
        x_buf[0, j] = rows_j
        xf = rows_j.astype(jnp.float32)

        @pl.when(j == 0)
        def _():
            open_rows(xf, every)
            acc[...] = jnp.zeros_like(acc)
            csum[...] = jnp.zeros_like(csum)

        tally(xf, every, pivot[...])
        gain = jnp.broadcast_to(gain_ref[:, columns(j)].astype(jnp.float32), (LANES, width)).T
        gain = jnp.concatenate([gain] * (cols // LANES), axis=1)
        ones = jnp.ones((8, width), jnp.bfloat16)
        win_copy(j).wait()
        for i in range(3):
            scaled = (win_ref[i, columns(j), :].astype(jnp.float32) * gain).astype(jnp.bfloat16)
            win_ref[i, columns(j), :] = scaled
            at = slice(i * cols, (i + 1) * cols)
            csum[:, at] += jnp.dot(ones, scaled, preferred_element_type=jnp.float32)
            acc[:, at] += jnp.dot(rows_j, scaled, preferred_element_type=jnp.float32)
        return carry

    def unit(n, r, dz, dy):
        j = tp_at(dz, dy)
        at = pl.ds(r * half, half)
        block = x_buf[n, j, at]
        xf = block.astype(jnp.float32)
        if dz == 0 and dy == 0:
            open_rows(xf, at)
        tally(xf, at, pivot[at])
        for i in range(3):
            product = jnp.dot(block, win_ref[i, columns(j), :], preferred_element_type=jnp.float32)
            if dz == 0 and dy == 0:
                acc[at, i * cols:(i + 1) * cols] = product
            else:
                acc[at, i * cols:(i + 1) * cols] += product

    def gather_project(n):
        handed = passes(s, n)

        def take(r):
            @pl.when(handed)
            def _():
                forward_all(n, range(r * per_half, (r + 1) * per_half))

        def near(r):
            for dz in range(nz):
                unit(n, r, dz, 0)

        def across(r):
            for dz in range(nz):
                for h in range(r * per_half, (r + 1) * per_half):
                    when_full(n, h, functools.partial(arrive, n, h, dz))
                for dy in range(1, ny):
                    unit(n, r, dz, dy)

        blank(n)
        take(0)
        near(0)
        for r in range(1, HALVES):
            take(r)
            across(r - 1)
            near(r)
        across(HALVES - 1)

    def attend():
        m = jnp.sum(sum_1[...], axis=-1, keepdims=True) * (1.0 / count)
        var = jnp.maximum(jnp.sum(sum_2[...], axis=-1, keepdims=True) * (1.0 / count) - m * m, 0.0)
        mean = pivot[:, 0:1] + m
        rstd = lax.rsqrt(var + NORM_EPS)
        qkv[...] = ((acc[...] - mean * csum[0:1, :]) * rstd).astype(jnp.bfloat16)
        causal = lax.broadcasted_iota(jnp.int32, (rows, rows), 0) >= lax.broadcasted_iota(jnp.int32, (rows, rows), 1)
        for h in range(heads):
            q = qkv[:, h * HD:(h + 1) * HD]
            k = qkv[:, cols + h * HD:cols + (h + 1) * HD]
            v = qkv[:, 2 * cols + h * HD:2 * cols + (h + 1) * HD]
            scores = lax.dot_general(q, k, (((1,), (1,)), ((), ())), preferred_element_type=jnp.float32)
            scores = jnp.where(causal, scores * HD ** (-0.5), -jnp.inf)
            weights = jnp.exp(scores - jnp.max(scores, axis=-1, keepdims=True))
            probs = (weights / jnp.sum(weights, axis=-1, keepdims=True)).astype(jnp.bfloat16)
            ctx[:, h * HD:(h + 1) * HD] = jnp.dot(probs, v, preferred_element_type=jnp.float32).astype(jnp.bfloat16)

    def settled(section, h):
        early = (section < lost) | (section - TICKS + 1 > lost)
        return pick(early, y_buf[TICKS - 1, span(h)], y_buf[TICKS, span(h)])

    def send_spare(h):
        early = (s - 1 < lost) | (s - TICKS > lost)
        spare = pick(early, y_buf[TICKS, span(h)], y_buf[TICKS + 1, span(h)])
        spare = pick(s - 1 == lost, y_buf[1, span(h)], spare)
        spare_buf[span(h)] = pick(s == 0, y_buf[TICKS + 1, span(h)], spare)
        spare_copy(h).start()

    def write_later():
        @pl.when(s == 1)
        def _():
            for j in range(devices):
                rows_j = x_buf[TICKS, j]
                x_buf[steps, j] = pick(s == lost, jnp.zeros_like(rows_j), rows_j)

        @pl.when(s > 1)
        def _():
            behind = s - 1
            early = (behind != lost) & ((behind < lost) | (behind - TICKS + 1 > lost))
            for j in range(devices):
                rows_j = pick(early, x_buf[TICKS, j], x_buf[TICKS + 1, j])
                x_buf[steps, j] = pick(s == lost, jnp.zeros_like(rows_j), rows_j)

        @pl.when(s > 0)
        def _():
            for j in range(devices):
                later_copy(j).start()

    def project_out(n):
        def partial_for(tp):
            return jnp.dot(ctx[...], wout_ref[:, columns(tp)], preferred_element_type=jnp.float32)

        turn = n % 3
        def crossed(dy, h):
            return copy_to(part.at[dy - 1, :, span(h)], ry_buf.at[turn, dy - 1, :, span(h)],
                           rs_ys.at[0], rs_yr.at[turn, h, dy - 1], s, tp_at(0, dy))

        def summed(dz, h):
            return copy_to(zs_buf.at[dz - 1, span(h)], rz_buf.at[turn, dz - 1, span(h)],
                           rs_zs.at[0], rs_zr.at[turn, h, dz - 1], s, tp_at(dz, 0))

        def cross(h):
            for dy in range(1, ny):
                crossed(dy, h).start()

        for dz in far:
            for dy in range(1, ny):
                part[dy - 1, dz] = partial_for(tp_at(dz, dy)).astype(jnp.bfloat16)
        if sections <= TICKS + 1:
            @pl.when(follows(s, n))
            def _():
                pl.semaphore_wait(turn_sem, 1)

        for h in range(PIECES):
            when_full(n, h, functools.partial(cross, h))

        for tick, slot in pools:
            pl.when((s == 0) & (n == tick))(functools.partial(pool_forward, slot))

        for dz in far:
            own_part[dz] = partial_for(tp_at(dz, 0))

        @pl.when(n == TICKS + 1)
        def _():
            write_later()

        def over_y(h):
            for dy in range(1, ny):
                crossed(dy, h).wait_recv()
            for dz in far:
                total = own_part[dz, span(h)]
                for dy in range(1, ny):
                    total = total + ry_buf[turn, dy - 1, dz, span(h)].astype(jnp.float32)
                if dz:
                    zs_buf[dz - 1, span(h)] = total.astype(jnp.bfloat16)
                    summed(dz, h).start()
                else:
                    own_part[0, span(h)] = total

        def over_z(h):
            total = own_part[0, span(h)]
            for dz in range(1, nz):
                summed(dz, h).wait_recv()
                total = total + rz_buf[turn, dz - 1, span(h)].astype(jnp.float32)
            y_buf[n, span(h)] = (x_buf[n, me, span(h)].astype(jnp.float32) + total).astype(jnp.bfloat16)

            @pl.when((n < steps - 1) & passes(nxt, n + 1))
            def _():
                fwd_buf[n, span(h)] = y_buf[n, span(h)]

                @pl.when((n == TICKS) & (s == sections - 1))
                def _():
                    fwd_buf[n, span(h)] = pick(s == lost, y_buf[0, span(h)], settled(s, h))

                for dz in far:
                    fwd_copy(n, h, dz).start()

            @pl.when(n == TICKS + 1)
            def _():
                send_spare(h)

        for h in range(PIECES):
            when_full(n, h, functools.partial(over_y, h))
            if h == PIECES - 2:
                over_z(0)
        if sections <= TICKS + 1:
            @pl.when((s % 2 == 1) & follows(s - 1, n))
            def _():
                pl.semaphore_signal(turn_sem, inc=1, device_id={"section": prv, "tp": me}, device_id_type=MESH)

        for h in range(1, PIECES):
            when_full(n, h, functools.partial(over_z, h))

        @pl.when(jnp.logical_not(small(n)))
        def _():
            sent(part, rs_ys.at[0])
            sent(zs_buf, rs_zs.at[0])

        if sections <= TICKS + 1:
            @pl.when(small(n))
            def _():
                for h in range(1, PIECES):
                    y_buf[n, span(h)] = y_buf[n, span(0)]
                sent(part.at[:, :, span(0)], rs_ys.at[0])
                sent(zs_buf.at[:, span(0)], rs_zs.at[0])

    def step(n, carry):
        @pl.when(needed(s, n))
        def _():
            for tick, slot in pools:
                pl.when((s == 0) & (n == tick))(functools.partial(pool_start, slot, tick))

            @pl.when(n == 0)
            def _():
                lax.fori_loop(0, devices, first_rows, 0)
                wout_copy.wait()

            @pl.when(n > 0)
            def _():
                gather_project(n)

            attend()
            project_out(n)

        @pl.when(jnp.logical_not(needed(s, n)))
        def _():
            y_buf[n] = jnp.zeros((rows, width), jnp.bfloat16)

            @pl.when((s == 0) & (n == TICKS))
            def _():
                arrive_all(steps)
                for j in range(devices):
                    later_copy(j).start()

            @pl.when(n == TICKS + 1)
            def _():
                for h in range(PIECES):
                    send_spare(h)

                @pl.when(passes(s, n))
                def _():
                    forward_all(n, range(PIECES))
                    arrive_all(n)

                write_later()

        return carry

    pool_copy.wait()

    lax.fori_loop(0, steps, step, 0)

    def drain(n, carry):
        @pl.when(passes(nxt, n) & (n < steps))
        def _():
            sent_blocks(n - 1, nz, fw_s.at[n - 1])

        @pl.when(pooled(n))
        def _():
            sent(x_buf.at[n, pl.ds(0, nz - 1)], ag_zs.at[n - 1])

        @pl.when(pooled(n) | (passes(s, n) & (n < steps)))
        def _():
            sent_blocks(n, nz * (ny - 1), ag_ys.at[n - 1])

        return carry

    def standby_copy(h):
        return pltpu.make_async_copy(spare_in.at[span(h)], standby_hbm.at[0, span(h), :], w_sem.at[h])

    for h in range(PIECES):
        spare_copy(h).wait_recv()
        standby_copy(h).start()
    lax.fori_loop(1, steps + 1, drain, 0)
    for j in range(devices):
        later_copy(j).wait()
    sent(spare_buf, sp_s.at[0])
    for h in range(PIECES):
        standby_copy(h).wait()


def hand_out(later_hbm, standby_hbm, later_out, standby_out, later_buf, standby_buf, in_sem, out_sem):
    cut = later_buf.shape[1] // PIECES
    parts = [(later_hbm.at[:, pl.ds(h * cut, cut)], later_buf.at[:, pl.ds(h * cut, cut)],
              later_out.at[:, pl.ds(h * cut, cut)]) for h in range(PIECES)]
    parts.append((standby_hbm, standby_buf, standby_out))
    reads = [pltpu.make_async_copy(a, b, in_sem.at[k]) for k, (a, b, _) in enumerate(parts)]
    writes = [pltpu.make_async_copy(b, c, out_sem.at[k]) for k, (_, b, c) in enumerate(parts)]
    for copy in reads:
        copy.start()
    for read, write in zip(reads, writes):
        read.wait()
        write.start()
    for copy in writes:
        copy.wait()


def solution(mesh):
    sections, devices = mesh.shape["section"], mesh.shape["tp"]
    ny = 1
    while (2 * ny) * (2 * ny) <= devices and devices % (2 * ny) == 0:
        ny *= 2
    nz = devices // ny

    def per_device(pend, pool, plan, lost, win, wout, gain):
        rows, hidden = pend.shape[1], pend.shape[2]
        width = hidden // devices
        cols = win.shape[3]
        slots = TICKS + 3
        win = jnp.transpose(win[0], (1, 0, 2))
        vmem = pl.BlockSpec(memory_space=pltpu.VMEM)
        smem = pl.BlockSpec(memory_space=pltpu.SMEM)
        hbm = pl.BlockSpec(memory_space=pl.ANY)
        bf = functools.partial(pltpu.VMEM, dtype=jnp.bfloat16)
        fl = functools.partial(pltpu.VMEM, dtype=jnp.float32)
        dma = pltpu.SemaphoreType.DMA
        later, standby = pl.pallas_call(
            functools.partial(relay_kernel, sections, nz, ny),
            out_shape=(
                jax.ShapeDtypeStruct((1, rows, hidden), jnp.bfloat16),
                jax.ShapeDtypeStruct((1, rows, width), jnp.bfloat16),
            ),
            in_specs=[smem, smem, hbm, hbm, hbm, hbm, vmem],
            out_specs=(hbm, hbm),
            scratch_shapes=[
                bf((3, hidden, cols)),
                bf((cols, hidden)),
                bf(pool.shape),
                bf((slots, devices, rows, width)),
                bf((slots, rows, width)),
                fl((rows, LANES)), fl((rows, LANES)), fl((rows, LANES)),
                fl((8, 3 * cols)),
                fl((rows, 3 * cols)),
                bf((rows, 3 * cols)),
                bf((rows, cols)),
                bf((ny - 1, nz, rows, width)),
                fl((nz, rows, width)),
                bf((3, ny - 1, nz, rows, width)),
                bf((nz - 1, rows, width)),
                bf((3, nz - 1, rows, width)),
                bf((slots, rows, width)),
                bf((rows, width)),
                bf((rows, width)),
                dma((devices,)), dma((devices,)), dma((2,)),
                dma((slots - 1,)), dma((slots - 1,)), dma((slots - 1, PIECES, nz)),
                dma((slots - 1,)), dma((slots - 1, PIECES, nz, ny - 1)),
                dma((1,)), dma((3, PIECES, nz - 1)), dma((1,)), dma((3, PIECES, ny - 1)),
                dma((1,)), dma((PIECES,)), pltpu.SemaphoreType.REGULAR,
            ],
            compiler_params=pltpu.CompilerParams(
                collective_id=0, has_side_effects=True, vmem_limit_bytes=60 * 1024 * 1024
            ),
        )(lost, plan, pend, pool, win, wout[0], gain)
        return pl.pallas_call(
            hand_out,
            out_shape=(
                jax.ShapeDtypeStruct(later.shape, later.dtype),
                jax.ShapeDtypeStruct(standby.shape, standby.dtype),
            ),
            in_specs=[hbm, hbm],
            out_specs=(hbm, hbm),
            scratch_shapes=[bf(later.shape), bf(standby.shape), dma((PIECES + 1,)), dma((PIECES + 1,))],
        )(later, standby)

    placed = (
        P("section", None, None),
        P(None, None, "tp"),
        P(),
        P(),
        P("section", None, None, "tp"),
        P("section", "tp", None),
        P("section", None),
    )
    return jax.shard_map(
        per_device,
        mesh=mesh,
        in_specs=placed,
        out_specs=(P("section", None, None), P("section", None, "tp")),
        check_vma=False,
    )
```
